32 devices in a mesh: root: 4 (over z), virt: 4 (over y, x), occ: 2 (over core).
Axes of the slice: x: 2, y: 2, z: 4, core: 2. Of those that a mesh axis runs over, the one named last changes fastest.
Arguments:
- trial_singles: bfloat16 [8, 96], P('root'), may hold values from -6 to 6
- trial_doubles: bfloat16 [8, 480, 9216], P('root', 'virt', 'occ'), may hold values from -6 to 6
- occ_fock: bfloat16 [96, 96], replicated, may hold values from -0.625 to 0.625
- virt_fock: bfloat16 [480, 480], replicated, may hold values from -0.25 to 0.25
- w_ovoo: bfloat16 [96, 480, 9216], P('occ', 'virt', 'root'), may hold values from -0.625 to 0.625
- w_ooov: bfloat16 [96, 480, 9216], P('occ', 'virt', 'root'), may hold values from -0.0029296875 to 0.0029296875
- converged: int32 [8], replicated, may hold values from 0 to 1, as said below
Outputs:
- sigma_doubles: bfloat16 [8, 480, 9216], P('root', 'virt', 'occ')
- sigma_singles: float32 [8, 96], P('root')
- subspace: float32 [8, 8], P('root')
The draws below stay inside these ranges and needn't reach their ends.
Inputs may be any that keep to these rules, and one draw needn't show every extreme that they name: `converged`: exactly 4 roots are active (0). In every draw at least one aligned block of 2 roots has all its roots active; other blocks may have none.
All inputs are finite; a program needn't handle non-finite values.
Results may differ from the reference program's by a relative error of at most 0.0044.
Values may be sent and summed in bfloat16 or wider, within the bound.
A program may use at most 256 MiB of HBM per device.

```python
import math
import jax
import jax.numpy as jnp
from jax import lax

O = 96
V = 480
ROOTS_DEV = 2
ROOTS = 8


def draw_converged(key, part):
    groups = ROOTS // ROOTS_DEV
    level = jax.random.randint(jax.random.fold_in(key, 11), (groups,), 0, 4)
    chosen = jax.random.randint(jax.random.fold_in(key, 13), (), 0, groups)
    level = level.at[chosen].set(4)
    noise = jax.random.randint(jax.random.fold_in(key, 12), (ROOTS,), 0, ROOTS)
    positions = jnp.arange(ROOTS, dtype=jnp.int32)
    group_of = positions // ROOTS_DEV
    score = (level[group_of] * ROOTS + noise) * ROOTS + positions
    ranking = jnp.argsort(jnp.argsort(-score))
    return (ranking >= ROOTS // 2).astype(jnp.int32)


def levels(rng, dims, shards, low, high):
    def one(position, parts):
        draws = jax.random.uniform(jax.random.fold_in(jax.random.fold_in(rng, 6), position), (parts,), jnp.float32, low / len(shards), high / len(shards))
        return jnp.repeat(jnp.exp(draws), dims[position] // parts).reshape((-1,) + (1,) * (len(dims) - position - 1))

    gain = one(*shards[0])
    for cut in shards[1:]:
        gain = gain * one(*cut)
    return gain


def scatter_about(stream_key, extent, width, limit, cuts=(), kind=jnp.bfloat16):
    loudness = levels(stream_key, extent, cuts, -0.22, 0.18) if cuts else 1.0
    values = jax.random.normal(stream_key, extent, jnp.float32) * width * loudness
    return jnp.minimum(jnp.maximum(values, -limit), limit).astype(kind)


def setup_inputs(seed: int = 0) -> dict:
    streams_of = jax.random.split(jax.random.key(seed), 8)
    trial_singles = scatter_about(streams_of[0], (ROOTS, O), 1.0, 6.0, ((0, 4),))
    trial_doubles = scatter_about(streams_of[1], (ROOTS, V, O * O), 1.0, 6.0, ((0, 4), (1, 4), (2, 2)))
    occ_fock = scatter_about(streams_of[2], (O, O), O ** -0.5, 0.625)
    virt_fock = scatter_about(streams_of[3], (V, V), V ** -0.5, 0.25)
    w_ovoo = scatter_about(streams_of[4], (O, V, O * O), O ** -0.5, 0.625, ((0, 2), (1, 4), (2, 4)))
    w_ooov = scatter_about(streams_of[5], (O, V, O * O), (O * O * V) ** -0.5, 0.0029296875, ((0, 2), (1, 4), (2, 4)))
    converged = draw_converged(jax.random.fold_in(streams_of[7], 71), 0)
    return {"trial_singles": trial_singles, "trial_doubles": trial_doubles, "occ_fock": occ_fock, "virt_fock": virt_fock, "w_ovoo": w_ovoo, "w_ooov": w_ooov, "converged": converged}


def reference(trial_singles, trial_doubles, occ_fock, virt_fock, w_ovoo, w_ooov, converged):
    active = (1 - converged).astype(jnp.float32)
    outer_flat = w_ovoo.reshape(O, V * O * O)
    inner_flat = w_ooov.reshape(O, V * O * O)
    occ_wide = occ_fock.astype(jnp.float32)

    def per_root(bundle):
        single_row, double_block, weight_now = bundle
        outer_term = (-jnp.dot(single_row[None, :], outer_flat, preferred_element_type=jnp.float32)).reshape(V, O, O)
        vv_term = jnp.dot(virt_fock, double_block, preferred_element_type=jnp.float32).astype(jnp.bfloat16).reshape(V, O, O)
        block_wide = double_block.reshape(V, O, O).astype(jnp.float32)
        first_term = jnp.einsum('ki,akj->aij', occ_wide, block_wide)
        second_term = jnp.einsum('kj,aik->aij', occ_wide, block_wide)
        summed = weight_now * (vv_term.astype(jnp.float32) + outer_term - first_term - second_term)
        coupling = jnp.dot(inner_flat, double_block.reshape(V * O * O), preferred_element_type=jnp.float32)
        return (summed.reshape(V, O * O).astype(jnp.bfloat16), coupling)
    sigma_doubles, coupling = lax.map(per_root, (trial_singles, trial_doubles, active))
    singles_fock = jnp.dot(trial_singles, occ_fock, preferred_element_type=jnp.float32)
    sigma_singles = active[:, None] * (-singles_fock - 0.5 * coupling)
    doubles_part = jnp.dot(trial_doubles.reshape(ROOTS, V * O * O), sigma_doubles.reshape(ROOTS, V * O * O).T, preferred_element_type=jnp.float32)
    singles_part = jnp.dot(trial_singles.astype(jnp.float32), sigma_singles.T, precision=lax.Precision.HIGHEST)
    subspace = doubles_part / math.sqrt(O * O * V) + singles_part / math.sqrt(O)
    return (sigma_doubles, sigma_singles, subspace)
```

```python
import math

import jax
import jax.numpy as jnp
from jax import lax
from jax.experimental import pallas as pl
from jax.experimental.pallas import tpu as pltpu
from jax.sharding import PartitionSpec as P


def flat_pairs(left, right):
    return lax.dot_general(
        left.reshape(left.shape[0], -1),
        right.reshape(right.shape[0], -1),
        (((1,), (1,)), ((), ())),
        preferred_element_type=jnp.float32,
    )


def plain(trial_singles, trial_doubles, occ_fock, virt_fock, w_ovoo, w_ooov, converged):
    local_roots, virt_local, pair_local = trial_doubles.shape
    occ_count = occ_fock.shape[0]
    virt_count = virt_fock.shape[0]
    root_count = converged.shape[0]
    root_groups = lax.axis_size("root")
    occ_groups = lax.axis_size("occ")
    root_index = lax.axis_index("root")
    occ_index = lax.axis_index("occ")
    occ_half = occ_count // occ_groups
    block_pairs = occ_count * occ_count // root_groups
    own_start = occ_index * occ_half
    active = (1 - converged).astype(jnp.float32)
    own_active = lax.dynamic_slice_in_dim(active, root_index * local_roots, local_roots)
    singles_all = lax.all_gather(trial_singles, "root", axis=0, tiled=True)
    gathered = lax.all_gather(trial_doubles, "occ", axis=2, tiled=True)
    fock_cols = lax.dynamic_slice_in_dim(occ_fock, own_start, occ_half, 1)
    batch_rows = local_roots * virt_local
    stacked = gathered.reshape(batch_rows, occ_count, occ_count)
    first_term = jnp.einsum(
        "ki,bkj->bij", fock_cols, stacked, preferred_element_type=jnp.float32
    ).reshape(local_roots, virt_local, pair_local)
    own_rows = trial_doubles.reshape(batch_rows, occ_half, occ_count)
    second_term = jnp.einsum(
        "bik,kj->bij", own_rows, occ_fock, preferred_element_type=jnp.float32
    ).reshape(local_roots, virt_local, pair_local)
    doubles_block = lax.all_to_all(gathered, "root", split_axis=2, concat_axis=0, tiled=True)
    partial_coupling = flat_pairs(doubles_block, w_ooov)
    coupling_part = lax.dynamic_update_slice(
        jnp.zeros((root_count, occ_count), jnp.float32), partial_coupling, (jnp.int32(0), own_start)
    )
    coupling = lax.psum(coupling_part, ("root", "virt", "occ"))
    singles_fock = jnp.dot(singles_all, occ_fock, preferred_element_type=jnp.float32)
    singles_every = active[:, None] * (-singles_fock - 0.5 * coupling)
    sigma_singles = lax.dynamic_slice_in_dim(singles_every, root_index * local_roots, local_roots)
    singles_cols = lax.dynamic_slice_in_dim(singles_all, own_start, occ_half, 1)
    outer_part = (
        -jnp.dot(singles_cols, w_ovoo.reshape(occ_half, -1), preferred_element_type=jnp.float32)
    ).reshape(root_count, virt_local, block_pairs)
    product = jnp.einsum(
        "ac,ncp->nap",
        virt_fock,
        lax.all_to_all(trial_doubles, "virt", split_axis=2, concat_axis=1, tiled=True),
        preferred_element_type=jnp.float32,
    ).astype(jnp.bfloat16)
    vv_term = lax.all_to_all(product, "virt", split_axis=1, concat_axis=2, tiled=True)
    vv_value = vv_term.astype(jnp.float32)
    outer_own = lax.all_to_all(outer_part, "root", split_axis=0, concat_axis=2, tiled=True)
    outer_half = lax.psum_scatter(outer_own, "occ", scatter_dimension=2, tiled=True)
    summed = vv_value + outer_half - first_term - second_term
    sigma_doubles = (own_active[:, None, None] * summed).astype(jnp.bfloat16)
    trial_piece, sigma_piece = (
        lax.all_to_all(trial_doubles, "root", split_axis=2, concat_axis=0, tiled=True),
        lax.all_to_all(sigma_doubles, "root", split_axis=2, concat_axis=0, tiled=True),
    )
    doubles_part = lax.psum(flat_pairs(trial_piece, sigma_piece), ("root", "virt", "occ"))
    singles_part = jnp.dot(
        singles_all.astype(jnp.float32), singles_every.T, precision=lax.Precision.HIGHEST
    )
    whole_matrix = doubles_part / math.sqrt(
        occ_count * occ_count * virt_count
    ) + singles_part / math.sqrt(occ_count)
    subspace = lax.dynamic_slice_in_dim(whole_matrix, root_index * local_roots, local_roots, 0)
    return (sigma_doubles, sigma_singles, subspace)


ROWS = 8


def call(body, grid, ins, outs, shapes, scratch=(), flops=0, moved=0, semantics=None):
    return pl.pallas_call(
        body,
        grid=grid,
        in_specs=ins,
        out_specs=outs,
        out_shape=shapes,
        scratch_shapes=list(scratch),
        compiler_params=pltpu.CompilerParams(
            dimension_semantics=("arbitrary",) * len(grid), vmem_limit_bytes=48 * 1024 * 1024
        ),
        cost_estimate=pl.CostEstimate(flops=flops, bytes_accessed=moved, transcendentals=0),
    )


SCALAR = pl.BlockSpec(memory_space=pltpu.SMEM)


def rows_flat(block):
    count, rows, width = block.shape
    return block.astype(jnp.float32).reshape(count * rows, width).astype(jnp.bfloat16)


def outer_body(core, mix, weights, kept, sent):
    roots, rows, width = kept.shape
    value = jnp.dot(mix[...], rows_flat(weights[...]), preferred_element_type=jnp.float32)
    value = value.reshape(roots, rows, 2 * width)
    low, high = value[:, :, :width], value[:, :, width:]
    first = core[0] == 0
    kept[...] = jnp.where(first, low, high)
    sent[...] = jnp.where(first, high, low).astype(jnp.bfloat16)


def outer_terms(core, singles_cols, weights):
    count, virt_local, pairs = weights.shape
    roots = singles_cols.shape[0]
    width = pairs // 2
    eye = jnp.eye(ROWS, dtype=jnp.bfloat16)
    mix = (-singles_cols[:, None, :, None] * eye[None, :, None, :]).reshape(
        roots * ROWS, count * ROWS
    )
    piece = pl.BlockSpec((roots, ROWS, width), lambda a: (0, a, 0))
    return call(
        outer_body,
        (virt_local // ROWS,),
        [
            SCALAR,
            pl.BlockSpec(mix.shape, lambda a: (0, 0)),
            pl.BlockSpec((count, ROWS, pairs), lambda a: (0, a, 0)),
        ],
        [piece, piece],
        [
            jax.ShapeDtypeStruct((roots, virt_local, width), jnp.float32),
            jax.ShapeDtypeStruct((roots, virt_local, width), jnp.bfloat16),
        ],
        flops=2 * roots * ROWS * weights.size,
        moved=2 * weights.size,
    )(core, mix, weights)


def coupling_body(core, own, other, weights, total, held):
    width = own.shape[2]

    @pl.when(pl.program_id(0) == 0)
    def _():
        held[...] = jnp.zeros_like(held)

    here = pl.multiple_of(core[0] * width, 128)
    there = pl.multiple_of((1 - core[0]) * width, 128)
    dims = (((1,), (1,)), ((), ()))
    held[...] += lax.dot_general(
        rows_flat(own[...]), rows_flat(weights[:, :, pl.ds(here, width)]), dims,
        preferred_element_type=jnp.float32,
    ) + lax.dot_general(
        rows_flat(other[...]), rows_flat(weights[:, :, pl.ds(there, width)]), dims,
        preferred_element_type=jnp.float32,
    )

    @pl.when(pl.program_id(0) == pl.num_programs(0) - 1)
    def _():
        total[...] = held[...]


def same_row(table, left, rows, right):
    eye = jnp.eye(rows, dtype=jnp.float32)
    return jnp.sum(table.reshape(left, rows, right, rows) * eye[None, :, None, :], axis=(1, 3))


def coupling_sums(core, own, other, weights):
    count, virt_local, pairs = weights.shape
    roots, _, width = own.shape
    shape = (roots * ROWS, count * ROWS)
    piece = pl.BlockSpec((roots, ROWS, width), lambda a: (0, a, 0))
    table = call(
        coupling_body,
        (virt_local // ROWS,),
        [SCALAR, piece, piece, pl.BlockSpec((count, ROWS, pairs), lambda a: (0, a, 0))],
        pl.BlockSpec(shape, lambda a: (0, 0)),
        jax.ShapeDtypeStruct(shape, jnp.float32),
        [pltpu.VMEM(shape, jnp.float32)],
        flops=2 * roots * ROWS * weights.size,
        moved=2 * weights.size,
    )(core, own, other, weights)
    return same_row(table, roots, ROWS, count)


def project_body(left, right, total, held):
    @pl.when(pl.program_id(0) == 0)
    def _():
        held[...] = jnp.zeros_like(held)

    held[...] += lax.dot_general(
        rows_flat(left[...]), rows_flat(right[...]), (((1,), (1,)), ((), ())),
        preferred_element_type=jnp.float32,
    )

    @pl.when(pl.program_id(0) == pl.num_programs(0) - 1)
    def _():
        total[...] = held[...]


def project(left, right):
    roots, virt_local, width = left.shape
    rows = next(n for n in (40, 24, 16, 8) if virt_local % n == 0)
    shape = (roots * rows, roots * rows)
    piece = pl.BlockSpec((roots, rows, width), lambda a: (0, a, 0))
    table = call(
        project_body,
        (virt_local // rows,),
        [piece, piece],
        pl.BlockSpec(shape, lambda a: (0, 0)),
        jax.ShapeDtypeStruct(shape, jnp.float32),
        [pltpu.VMEM(shape, jnp.float32)],
        flops=2 * roots * rows * left.size,
        moved=4 * left.size,
    )(left, right)
    return same_row(table, roots, rows, roots)


def occ_body(tile, count, own, other, own_fock, other_fock, unit, second, out):
    column = pl.program_id(0)

    def spread(rows):
        parts = [unit[...] * rows[k : k + 1, :] for k in range(rows.shape[0])]
        return jnp.concatenate(parts, axis=0).astype(jnp.bfloat16)

    def step(k, total):
        cut = pl.ds(pl.multiple_of(k * tile, 128), tile)
        total = total + jnp.dot(
            own[:, cut], spread(own_fock[k]), preferred_element_type=jnp.float32
        )
        return total + jnp.dot(
            other[:, cut], spread(other_fock[k]), preferred_element_type=jnp.float32
        )

    here = pl.ds(pl.multiple_of(column * tile, 128), tile)
    begin = jnp.dot(own[:, here], second[...], preferred_element_type=jnp.float32)
    out[...] = lax.fori_loop(0, count, step, begin)


def occ_terms(own, other, fock_own, fock_other, occ_fock):
    rows, pairs = own.shape
    occ_count = occ_fock.shape[0]
    group = 128 // math.gcd(occ_count, 128)
    tile = group * occ_count
    count = pairs // tile
    eye = jnp.eye(occ_count, dtype=jnp.float32)
    unit = jnp.tile(eye, (1, group))
    second = (
        jnp.eye(group, dtype=jnp.bfloat16)[:, None, :, None] * occ_fock[None, :, None, :]
    ).reshape(tile, tile)

    def wide(block):
        return jnp.repeat(block.astype(jnp.float32), occ_count, axis=1).reshape(count, group, pairs)

    whole = pl.BlockSpec((rows, pairs), lambda c: (0, 0))
    fock_spec = pl.BlockSpec((count, group, tile), lambda c: (0, 0, c))

    def body(*refs):
        occ_body(tile, count, *refs)

    return call(
        body,
        (count,),
        [
            whole,
            whole,
            fock_spec,
            fock_spec,
            pl.BlockSpec(unit.shape, lambda c: (0, 0)),
            pl.BlockSpec(second.shape, lambda c: (0, 0)),
        ],
        pl.BlockSpec((rows, tile), lambda c: (0, c)),
        jax.ShapeDtypeStruct((rows, pairs), jnp.float32),
        flops=4 * rows * pairs * pairs,
        moved=8 * rows * pairs,
    )(own, other, wide(fock_own), wide(fock_other), unit, second)


def virt_body(fock, amps, out):
    blocks = amps.shape[0]
    for b in range(blocks):
        total = jnp.dot(fock[b, 0], amps[0, 0], preferred_element_type=jnp.float32)
        for c in range(1, blocks):
            total += jnp.dot(fock[b, c], amps[c, 0], preferred_element_type=jnp.float32)
        out[b, 0] = total.astype(jnp.bfloat16)


def virt_product(virt_fock, amps):
    blocks, roots, virt_local, width = amps.shape
    fock = virt_fock.reshape(blocks, virt_local, blocks, virt_local).transpose(0, 2, 1, 3)
    piece = pl.BlockSpec((blocks, 1, virt_local, width), lambda n: (0, n, 0, 0))
    return call(
        virt_body,
        (roots,),
        [pl.BlockSpec(fock.shape, lambda n: (0, 0, 0, 0)), piece],
        piece,
        jax.ShapeDtypeStruct(amps.shape, jnp.bfloat16),
        flops=2 * blocks * virt_local * amps.size,
        moved=4 * amps.size,
    )(fock, amps)


def sigma_body(core, active, vv, mine, theirs, occ_sum, sigma, kept, sent):
    width = mine.shape[3]
    first = core[0] == 0
    weight = active[pl.program_id(0)]
    here = mine[0, 0].astype(jnp.float32)
    there = theirs[0, 0].astype(jnp.float32)
    low = vv[0, 0].astype(jnp.float32) + jnp.where(first, here, there) - occ_sum[0, :, :width]
    high = vv[1, 0].astype(jnp.float32) + jnp.where(first, there, here) - occ_sum[0, :, width:]
    low = weight * low
    high = weight * high
    sigma[0, :, :width] = low.astype(jnp.bfloat16)
    sigma[0, :, width:] = high.astype(jnp.bfloat16)
    kept[0, 0] = jnp.where(first, low, high).astype(jnp.bfloat16)
    sent[0, 0] = jnp.where(first, high, low).astype(jnp.bfloat16)


def sigma_terms(core, active, vv, mine, theirs, occ_sum):
    quarters, roots, virt_local, width = mine.shape
    piece = pl.BlockSpec((1, 1, virt_local, width), lambda n, q: (q, n, 0, 0))
    full = pl.BlockSpec((1, virt_local, 2 * width), lambda n, q: (n, 0, q))
    return call(
        sigma_body,
        (roots, quarters),
        [
            SCALAR,
            SCALAR,
            pl.BlockSpec((2, 1, virt_local, width), lambda n, q: (q, n, 0, 0)),
            piece,
            piece,
            full,
        ],
        [full, piece, piece],
        [
            jax.ShapeDtypeStruct(occ_sum.shape, jnp.bfloat16),
            jax.ShapeDtypeStruct(mine.shape, jnp.bfloat16),
            jax.ShapeDtypeStruct(mine.shape, jnp.bfloat16),
        ],
        flops=8 * occ_sum.size,
        moved=14 * occ_sum.size,
    )(core, active, vv, mine, theirs, occ_sum)


def tiled(trial_doubles, virt_fock, occ_fock):
    _, virt_local, pair_local = trial_doubles.shape
    occ_count = occ_fock.shape[0]
    root_groups = lax.axis_size("root")
    sub = occ_count * occ_count // root_groups // 2
    tile = occ_count * 128 // math.gcd(occ_count, 128)
    return (
        lax.axis_size("occ") == 2
        and root_groups % 2 == 0
        and virt_local % ROWS == 0
        and sub % 128 == 0
        and sub * lax.axis_size("virt") == pair_local
        and pair_local % tile == 0
    )


def local(trial_singles, trial_doubles, occ_fock, virt_fock, w_ovoo, w_ooov, converged):
    if not tiled(trial_doubles, virt_fock, occ_fock):
        return plain(trial_singles, trial_doubles, occ_fock, virt_fock, w_ovoo, w_ooov, converged)
    local_roots, virt_local, pair_local = trial_doubles.shape
    occ_count = occ_fock.shape[0]
    virt_count = virt_fock.shape[0]
    root_count = converged.shape[0]
    root_groups = lax.axis_size("root")
    virt_groups = lax.axis_size("virt")
    root_index = lax.axis_index("root")
    occ_index = lax.axis_index("occ")
    occ_half = occ_count // 2
    quarters = root_groups // 2
    sub = pair_local // quarters // 2
    own_start = occ_index * occ_half
    other_start = (1 - occ_index) * occ_half
    core = occ_index.astype(jnp.int32).reshape(1)
    first_core = occ_index == 0
    active = (1 - converged).astype(jnp.float32)
    own_active = lax.dynamic_slice_in_dim(active, root_index * local_roots, local_roots)

    def swap(value):
        return lax.ppermute(value, "occ", [(0, 1), (1, 0)])

    def exchange(value, axis):
        return lax.all_to_all(value, axis, split_axis=0, concat_axis=0, tiled=True)

    def in_order(kept, got):
        return jnp.concatenate(
            [jnp.where(first_core, kept, got), jnp.where(first_core, got, kept)], axis=0
        )

    def own_subs(value):
        return jnp.stack(
            [
                lax.dynamic_slice_in_dim(value, 2 * q * sub + occ_index * sub, sub, 2)
                for q in range(quarters)
            ]
        )

    singles_all = lax.all_gather(trial_singles, "root", axis=0, tiled=True)
    other_doubles = swap(trial_doubles)
    trial_piece = exchange(in_order(own_subs(trial_doubles), own_subs(other_doubles)), "root")
    trial_piece = trial_piece.reshape(root_count, virt_local, sub)
    slabs = jnp.stack(jnp.split(trial_doubles, virt_groups, axis=2))
    slabs = exchange(slabs, "virt")

    singles_cols = lax.dynamic_slice_in_dim(singles_all, own_start, occ_half, 1)
    outer_kept, outer_sent = outer_terms(core, singles_cols, w_ovoo)
    outer_sum = (outer_kept + swap(outer_sent).astype(jnp.float32)).astype(jnp.bfloat16)
    outer_quarters = exchange(
        outer_sum.reshape(root_groups, local_roots, virt_local, sub), "root"
    )

    fock_cols = lax.dynamic_slice_in_dim(occ_fock, own_start, occ_half, 1)
    occ_sum = occ_terms(
        trial_doubles.reshape(local_roots * virt_local, pair_local),
        other_doubles.reshape(local_roots * virt_local, pair_local),
        lax.dynamic_slice_in_dim(fock_cols, own_start, occ_half, 0),
        lax.dynamic_slice_in_dim(fock_cols, other_start, occ_half, 0),
        occ_fock,
    ).reshape(local_roots, virt_local, pair_local)
    vv_term = exchange(virt_product(virt_fock, slabs), "virt")

    partial_coupling = coupling_sums(core, trial_piece, swap(trial_piece), w_ooov)
    coupling_part = lax.dynamic_update_slice(
        jnp.zeros((root_count, occ_count), jnp.float32), partial_coupling, (jnp.int32(0), own_start)
    )

    outer_mine = lax.dynamic_slice_in_dim(outer_quarters, quarters * occ_index, quarters)
    outer_theirs = swap(
        lax.dynamic_slice_in_dim(outer_quarters, quarters * (1 - occ_index), quarters)
    )
    sigma_doubles, sigma_kept, sigma_sent = sigma_terms(
        core, own_active, vv_term, outer_mine, outer_theirs, occ_sum
    )
    sigma_piece = exchange(in_order(sigma_kept, swap(sigma_sent)), "root")
    doubles_piece = project(trial_piece, sigma_piece.reshape(root_count, virt_local, sub))

    coupling, doubles_part = lax.psum((coupling_part, doubles_piece), ("root", "virt", "occ"))
    singles_fock = jnp.dot(singles_all, occ_fock, preferred_element_type=jnp.float32)
    singles_every = active[:, None] * (-singles_fock - 0.5 * coupling)
    sigma_singles = lax.dynamic_slice_in_dim(singles_every, root_index * local_roots, local_roots)
    singles_part = jnp.dot(
        singles_all.astype(jnp.float32), singles_every.T, precision=lax.Precision.HIGHEST
    )
    whole_matrix = doubles_part / math.sqrt(
        occ_count * occ_count * virt_count
    ) + singles_part / math.sqrt(occ_count)
    subspace = lax.dynamic_slice_in_dim(whole_matrix, root_index * local_roots, local_roots, 0)
    return (sigma_doubles, sigma_singles, subspace)


def solution(mesh):
    placed = (
        P("root", None),
        P("root", "virt", "occ"),
        P(),
        P(),
        P("occ", "virt", "root"),
        P("occ", "virt", "root"),
        P(),
    )
    return jax.shard_map(
        local,
        mesh=mesh,
        in_specs=placed,
        out_specs=(P("root", "virt", "occ"), P("root", None), P("root", None)),
        check_vma=False,
    )
```

```python
import math

import jax
import jax.numpy as jnp
from jax import lax
from jax.experimental import pallas as pl
from jax.experimental.pallas import tpu as pltpu
from jax.sharding import PartitionSpec as P


def flat_pairs(left, right):
    return lax.dot_general(
        left.reshape(left.shape[0], -1),
        right.reshape(right.shape[0], -1),
        (((1,), (1,)), ((), ())),
        preferred_element_type=jnp.float32,
    )


def plain(trial_singles, trial_doubles, occ_fock, virt_fock, w_ovoo, w_ooov, converged):
    local_roots, virt_local, pair_local = trial_doubles.shape
    occ_count = occ_fock.shape[0]
    virt_count = virt_fock.shape[0]
    root_count = converged.shape[0]
    root_groups = lax.axis_size("root")
    occ_groups = lax.axis_size("occ")
    root_index = lax.axis_index("root")
    occ_index = lax.axis_index("occ")
    occ_half = occ_count // occ_groups
    block_pairs = occ_count * occ_count // root_groups
    own_start = occ_index * occ_half
    active = (1 - converged).astype(jnp.float32)
    own_active = lax.dynamic_slice_in_dim(active, root_index * local_roots, local_roots)
    singles_all = lax.all_gather(trial_singles, "root", axis=0, tiled=True)
    gathered = lax.all_gather(trial_doubles, "occ", axis=2, tiled=True)
    fock_cols = lax.dynamic_slice_in_dim(occ_fock, own_start, occ_half, 1)
    batch_rows = local_roots * virt_local
    stacked = gathered.reshape(batch_rows, occ_count, occ_count)
    first_term = jnp.einsum(
        "ki,bkj->bij", fock_cols, stacked, preferred_element_type=jnp.float32
    ).reshape(local_roots, virt_local, pair_local)
    own_rows = trial_doubles.reshape(batch_rows, occ_half, occ_count)
    second_term = jnp.einsum(
        "bik,kj->bij", own_rows, occ_fock, preferred_element_type=jnp.float32
    ).reshape(local_roots, virt_local, pair_local)
    doubles_block = lax.all_to_all(gathered, "root", split_axis=2, concat_axis=0, tiled=True)
    partial_coupling = flat_pairs(doubles_block, w_ooov)
    coupling_part = lax.dynamic_update_slice(
        jnp.zeros((root_count, occ_count), jnp.float32), partial_coupling, (jnp.int32(0), own_start)
    )
    coupling = lax.psum(coupling_part, ("root", "virt", "occ"))
    singles_fock = jnp.dot(singles_all, occ_fock, preferred_element_type=jnp.float32)
    singles_every = active[:, None] * (-singles_fock - 0.5 * coupling)
    sigma_singles = lax.dynamic_slice_in_dim(singles_every, root_index * local_roots, local_roots)
    singles_cols = lax.dynamic_slice_in_dim(singles_all, own_start, occ_half, 1)
    outer_part = (
        -jnp.dot(singles_cols, w_ovoo.reshape(occ_half, -1), preferred_element_type=jnp.float32)
    ).reshape(root_count, virt_local, block_pairs)
    product = jnp.einsum(
        "ac,ncp->nap",
        virt_fock,
        lax.all_to_all(trial_doubles, "virt", split_axis=2, concat_axis=1, tiled=True),
        preferred_element_type=jnp.float32,
    ).astype(jnp.bfloat16)
    vv_term = lax.all_to_all(product, "virt", split_axis=1, concat_axis=2, tiled=True)
    vv_value = vv_term.astype(jnp.float32)
    outer_own = lax.all_to_all(outer_part, "root", split_axis=0, concat_axis=2, tiled=True)
    outer_half = lax.psum_scatter(outer_own, "occ", scatter_dimension=2, tiled=True)
    summed = vv_value + outer_half - first_term - second_term
    sigma_doubles = (own_active[:, None, None] * summed).astype(jnp.bfloat16)
    trial_piece, sigma_piece = (
        lax.all_to_all(trial_doubles, "root", split_axis=2, concat_axis=0, tiled=True),
        lax.all_to_all(sigma_doubles, "root", split_axis=2, concat_axis=0, tiled=True),
    )
    doubles_part = lax.psum(flat_pairs(trial_piece, sigma_piece), ("root", "virt", "occ"))
    singles_part = jnp.dot(
        singles_all.astype(jnp.float32), singles_every.T, precision=lax.Precision.HIGHEST
    )
    whole_matrix = doubles_part / math.sqrt(
        occ_count * occ_count * virt_count
    ) + singles_part / math.sqrt(occ_count)
    subspace = lax.dynamic_slice_in_dim(whole_matrix, root_index * local_roots, local_roots, 0)
    return (sigma_doubles, sigma_singles, subspace)


ROWS = 8


def call(body, grid, ins, outs, shapes, scratch=(), flops=0, moved=0, semantics=None):
    return pl.pallas_call(
        body,
        grid=grid,
        in_specs=ins,
        out_specs=outs,
        out_shape=shapes,
        scratch_shapes=list(scratch),
        compiler_params=pltpu.CompilerParams(
            dimension_semantics=("arbitrary",) * len(grid), vmem_limit_bytes=48 * 1024 * 1024
        ),
        cost_estimate=pl.CostEstimate(flops=flops, bytes_accessed=moved, transcendentals=0),
    )


SCALAR = pl.BlockSpec(memory_space=pltpu.SMEM)


def rows_flat(block):
    count, rows, width = block.shape
    return block.astype(jnp.float32).reshape(count * rows, width).astype(jnp.bfloat16)


def outer_body(core, mix, weights, kept, sent):
    roots, rows, width = kept.shape
    value = jnp.dot(mix[...], rows_flat(weights[...]), preferred_element_type=jnp.float32)
    value = value.reshape(roots, rows, 2 * width)
    low, high = value[:, :, :width], value[:, :, width:]
    first = core[0] == 0
    kept[...] = jnp.where(first, low, high)
    sent[...] = jnp.where(first, high, low).astype(jnp.bfloat16)


def outer_terms(core, singles_cols, weights):
    count, virt_local, pairs = weights.shape
    roots = singles_cols.shape[0]
    width = pairs // 2
    eye = jnp.eye(ROWS, dtype=jnp.bfloat16)
    mix = (-singles_cols[:, None, :, None] * eye[None, :, None, :]).reshape(
        roots * ROWS, count * ROWS
    )
    piece = pl.BlockSpec((roots, ROWS, width), lambda a: (0, a, 0))
    return call(
        outer_body,
        (virt_local // ROWS,),
        [
            SCALAR,
            pl.BlockSpec(mix.shape, lambda a: (0, 0)),
            pl.BlockSpec((count, ROWS, pairs), lambda a: (0, a, 0)),
        ],
        [piece, piece],
        [
            jax.ShapeDtypeStruct((roots, virt_local, width), jnp.float32),
            jax.ShapeDtypeStruct((roots, virt_local, width), jnp.bfloat16),
        ],
        flops=2 * roots * ROWS * weights.size,
        moved=2 * weights.size,
    )(core, mix, weights)


def coupling_body(core, own, other, weights, total, held):
    width = own.shape[2]

    @pl.when(pl.program_id(0) == 0)
    def _():
        held[...] = jnp.zeros_like(held)

    here = pl.multiple_of(core[0] * width, 128)
    there = pl.multiple_of((1 - core[0]) * width, 128)
    dims = (((1,), (1,)), ((), ()))
    held[...] += lax.dot_general(
        rows_flat(own[...]), rows_flat(weights[:, :, pl.ds(here, width)]), dims,
        preferred_element_type=jnp.float32,
    ) + lax.dot_general(
        rows_flat(other[...]), rows_flat(weights[:, :, pl.ds(there, width)]), dims,
        preferred_element_type=jnp.float32,
    )

    @pl.when(pl.program_id(0) == pl.num_programs(0) - 1)
    def _():
        total[...] = held[...]


def same_row(table, left, rows, right):
    eye = jnp.eye(rows, dtype=jnp.float32)
    return jnp.sum(table.reshape(left, rows, right, rows) * eye[None, :, None, :], axis=(1, 3))


def coupling_sums(core, own, other, weights):
    count, virt_local, pairs = weights.shape
    roots, _, width = own.shape
    shape = (roots * ROWS, count * ROWS)
    piece = pl.BlockSpec((roots, ROWS, width), lambda a: (0, a, 0))
    table = call(
        coupling_body,
        (virt_local // ROWS,),
        [SCALAR, piece, piece, pl.BlockSpec((count, ROWS, pairs), lambda a: (0, a, 0))],
        pl.BlockSpec(shape, lambda a: (0, 0)),
        jax.ShapeDtypeStruct(shape, jnp.float32),
        [pltpu.VMEM(shape, jnp.float32)],
        flops=2 * roots * ROWS * weights.size,
        moved=2 * weights.size,
    )(core, own, other, weights)
    return same_row(table, roots, ROWS, count)


def project_body(left, right, total, held):
    @pl.when(pl.program_id(0) == 0)
    def _():
        held[...] = jnp.zeros_like(held)

    held[...] += lax.dot_general(
        rows_flat(left[...]), rows_flat(right[...]), (((1,), (1,)), ((), ())),
        preferred_element_type=jnp.float32,
    )

    @pl.when(pl.program_id(0) == pl.num_programs(0) - 1)
    def _():
        total[...] = held[...]


def project(left, right):
    roots, virt_local, width = left.shape
    rows = next(n for n in (40, 24, 16, 8) if virt_local % n == 0)
    shape = (roots * rows, roots * rows)
    piece = pl.BlockSpec((roots, rows, width), lambda a: (0, a, 0))
    table = call(
        project_body,
        (virt_local // rows,),
        [piece, piece],
        pl.BlockSpec(shape, lambda a: (0, 0)),
        jax.ShapeDtypeStruct(shape, jnp.float32),
        [pltpu.VMEM(shape, jnp.float32)],
        flops=2 * roots * rows * left.size,
        moved=4 * left.size,
    )(left, right)
    return same_row(table, roots, rows, roots)


def occ_body(tile, count, first, own, other, own_fock, other_fock, unit, second, out):
    column = pl.program_id(0) + first

    def spread(rows):
        parts = [unit[...] * rows[k : k + 1, :] for k in range(rows.shape[0])]
        return jnp.concatenate(parts, axis=0).astype(jnp.bfloat16)

    def step(k, total):
        cut = pl.ds(pl.multiple_of(k * tile, 128), tile)
        total = total + jnp.dot(
            own[:, cut], spread(own_fock[k]), preferred_element_type=jnp.float32
        )
        return total + jnp.dot(
            other[:, cut], spread(other_fock[k]), preferred_element_type=jnp.float32
        )

    here = pl.ds(pl.multiple_of(column * tile, 128), tile)
    begin = jnp.dot(own[:, here], second[...], preferred_element_type=jnp.float32)
    out[...] = lax.fori_loop(0, count, step, begin)


def occ_terms(own, other, fock_own, fock_other, occ_fock, part, parts):
    rows, pairs = own.shape
    occ_count = occ_fock.shape[0]
    group = 128 // math.gcd(occ_count, 128)
    tile = group * occ_count
    count = pairs // tile
    steps = count // parts
    first = part * steps
    eye = jnp.eye(occ_count, dtype=jnp.float32)
    unit = jnp.tile(eye, (1, group))
    second = (
        jnp.eye(group, dtype=jnp.bfloat16)[:, None, :, None] * occ_fock[None, :, None, :]
    ).reshape(tile, tile)

    def wide(block):
        return jnp.repeat(block.astype(jnp.float32), occ_count, axis=1).reshape(count, group, pairs)

    whole = pl.BlockSpec((rows, pairs), lambda c: (0, 0))
    fock_spec = pl.BlockSpec((count, group, tile), lambda c: (0, 0, c + first))

    def body(*refs):
        occ_body(tile, count, first, *refs)

    return call(
        body,
        (steps,),
        [
            whole,
            whole,
            fock_spec,
            fock_spec,
            pl.BlockSpec(unit.shape, lambda c: (0, 0)),
            pl.BlockSpec(second.shape, lambda c: (0, 0)),
        ],
        pl.BlockSpec((rows, tile), lambda c: (0, c)),
        jax.ShapeDtypeStruct((rows, steps * tile), jnp.float32),
        flops=8 * rows * pairs * pairs // parts,
        moved=8 * rows * pairs,
    )(own, other, wide(fock_own), wide(fock_other), unit, second)


def virt_body(fock, amps, out):
    blocks = amps.shape[0]
    for b in range(blocks):
        total = jnp.dot(fock[b, 0], amps[0, 0], preferred_element_type=jnp.float32)
        for c in range(1, blocks):
            total += jnp.dot(fock[b, c], amps[c, 0], preferred_element_type=jnp.float32)
        out[b, 0] = total.astype(jnp.bfloat16)


def virt_product(virt_fock, amps):
    blocks, roots, virt_local, width = amps.shape
    fock = virt_fock.reshape(blocks, virt_local, blocks, virt_local).transpose(0, 2, 1, 3)
    piece = pl.BlockSpec((blocks, 1, virt_local, width), lambda n: (0, n, 0, 0))
    return call(
        virt_body,
        (roots,),
        [pl.BlockSpec(fock.shape, lambda n: (0, 0, 0, 0)), piece],
        piece,
        jax.ShapeDtypeStruct(amps.shape, jnp.bfloat16),
        flops=2 * blocks * virt_local * amps.size,
        moved=4 * amps.size,
    )(fock, amps)


def sigma_body(core, active, vv, mine, theirs, occ_sum, sigma, kept, sent):
    width = mine.shape[3]
    first = core[0] == 0
    weight = active[pl.program_id(0)]
    here = mine[0, 0].astype(jnp.float32)
    there = theirs[0, 0].astype(jnp.float32)
    low = vv[0, 0].astype(jnp.float32) + jnp.where(first, here, there) - occ_sum[0, :, :width]
    high = vv[1, 0].astype(jnp.float32) + jnp.where(first, there, here) - occ_sum[0, :, width:]
    low = weight * low
    high = weight * high
    sigma[0, :, :width] = low.astype(jnp.bfloat16)
    sigma[0, :, width:] = high.astype(jnp.bfloat16)
    kept[0, 0] = jnp.where(first, low, high).astype(jnp.bfloat16)
    sent[0, 0] = jnp.where(first, high, low).astype(jnp.bfloat16)


def sigma_terms(core, active, vv, mine, theirs, occ_sum):
    quarters, roots, virt_local, width = mine.shape
    piece = pl.BlockSpec((1, 1, virt_local, width), lambda n, q: (q, n, 0, 0))
    full = pl.BlockSpec((1, virt_local, 2 * width), lambda n, q: (n, 0, q))
    return call(
        sigma_body,
        (roots, quarters),
        [
            SCALAR,
            SCALAR,
            pl.BlockSpec((2, 1, virt_local, width), lambda n, q: (q, n, 0, 0)),
            piece,
            piece,
            full,
        ],
        [full, piece, piece],
        [
            jax.ShapeDtypeStruct(occ_sum.shape, jnp.bfloat16),
            jax.ShapeDtypeStruct(mine.shape, jnp.bfloat16),
            jax.ShapeDtypeStruct(mine.shape, jnp.bfloat16),
        ],
        flops=8 * occ_sum.size,
        moved=14 * occ_sum.size,
    )(core, active, vv, mine, theirs, occ_sum)


def tiled(trial_doubles, virt_fock, occ_fock):
    _, virt_local, pair_local = trial_doubles.shape
    occ_count = occ_fock.shape[0]
    root_groups = lax.axis_size("root")
    sub = occ_count * occ_count // root_groups // 2
    tile = occ_count * 128 // math.gcd(occ_count, 128)
    return (
        lax.axis_size("occ") == 2
        and root_groups % 2 == 0
        and virt_local % ROWS == 0
        and sub % 128 == 0
        and sub * lax.axis_size("virt") == pair_local
        and pair_local % (2 * tile) == 0
    )


def local(trial_singles, trial_doubles, occ_fock, virt_fock, w_ovoo, w_ooov, converged):
    if not tiled(trial_doubles, virt_fock, occ_fock):
        return plain(trial_singles, trial_doubles, occ_fock, virt_fock, w_ovoo, w_ooov, converged)
    local_roots, virt_local, pair_local = trial_doubles.shape
    occ_count = occ_fock.shape[0]
    virt_count = virt_fock.shape[0]
    root_count = converged.shape[0]
    root_groups = lax.axis_size("root")
    virt_groups = lax.axis_size("virt")
    root_index = lax.axis_index("root")
    occ_index = lax.axis_index("occ")
    occ_half = occ_count // 2
    quarters = root_groups // 2
    sub = pair_local // quarters // 2
    own_start = occ_index * occ_half
    other_start = (1 - occ_index) * occ_half
    core = occ_index.astype(jnp.int32).reshape(1)
    first_core = occ_index == 0
    active = (1 - converged).astype(jnp.float32)
    own_active = lax.dynamic_slice_in_dim(active, root_index * local_roots, local_roots)

    def swap(value):
        return lax.ppermute(value, "occ", [(0, 1), (1, 0)])

    def exchange(value, axis):
        return lax.all_to_all(value, axis, split_axis=0, concat_axis=0, tiled=True)

    def in_order(kept, got):
        return jnp.concatenate(
            [jnp.where(first_core, kept, got), jnp.where(first_core, got, kept)], axis=0
        )

    def own_subs(value):
        return jnp.stack(
            [
                lax.dynamic_slice_in_dim(value, 2 * q * sub + occ_index * sub, sub, 2)
                for q in range(quarters)
            ]
        )

    singles_all = lax.all_gather(trial_singles, "root", axis=0, tiled=True)
    other_doubles = swap(trial_doubles)
    trial_piece = exchange(in_order(own_subs(trial_doubles), own_subs(other_doubles)), "root")
    trial_piece = trial_piece.reshape(root_count, virt_local, sub)
    slabs = jnp.stack(jnp.split(trial_doubles, virt_groups, axis=2))
    slabs = exchange(slabs, "virt")

    singles_cols = lax.dynamic_slice_in_dim(singles_all, own_start, occ_half, 1)
    outer_kept, outer_sent = outer_terms(core, singles_cols, w_ovoo)
    outer_kept, outer_sent, slabs = lax.optimization_barrier((outer_kept, outer_sent, slabs))
    outer_sum = (outer_kept + swap(outer_sent).astype(jnp.float32)).astype(jnp.bfloat16)
    fock_cols = lax.dynamic_slice_in_dim(occ_fock, own_start, occ_half, 1)
    outer_quarters = exchange(
        outer_sum.reshape(root_groups, local_roots, virt_local, sub), "root"
    )

    own_flat = trial_doubles.reshape(local_roots * virt_local, pair_local)
    other_flat = other_doubles.reshape(local_roots * virt_local, pair_local)

    def occ_part(cols, part):
        return occ_terms(
            own_flat,
            other_flat,
            lax.dynamic_slice_in_dim(cols, own_start, occ_half, 0),
            lax.dynamic_slice_in_dim(cols, other_start, occ_half, 0),
            occ_fock,
            part,
            2,
        )

    occ_low = occ_part(fock_cols, 0)
    product = virt_product(virt_fock, slabs)
    product, occ_low, outer_quarters = lax.optimization_barrier((product, occ_low, outer_quarters))
    vv_term = exchange(product, "virt")
    vv_term, fock_cols = lax.optimization_barrier((vv_term, fock_cols))
    occ_high = occ_part(fock_cols, 1)
    occ_sum = jnp.concatenate([occ_low, occ_high], axis=1)
    occ_sum = occ_sum.reshape(local_roots, virt_local, pair_local)

    partial_coupling = coupling_sums(core, trial_piece, swap(trial_piece), w_ooov)
    coupling_part = lax.dynamic_update_slice(
        jnp.zeros((root_count, occ_count), jnp.float32), partial_coupling, (jnp.int32(0), own_start)
    )

    outer_mine = lax.dynamic_slice_in_dim(outer_quarters, quarters * occ_index, quarters)
    outer_theirs = swap(
        lax.dynamic_slice_in_dim(outer_quarters, quarters * (1 - occ_index), quarters)
    )
    sigma_doubles, sigma_kept, sigma_sent = sigma_terms(
        core, own_active, vv_term, outer_mine, outer_theirs, occ_sum
    )
    sigma_piece = exchange(in_order(sigma_kept, swap(sigma_sent)), "root")
    doubles_piece = project(trial_piece, sigma_piece.reshape(root_count, virt_local, sub))

    partial = jnp.concatenate([coupling_part, doubles_piece], axis=1)
    partial = jnp.sum(lax.all_gather(partial, ("root", "virt", "occ")), axis=0)
    coupling, doubles_part = partial[:, :occ_count], partial[:, occ_count:]
    singles_fock = jnp.dot(singles_all, occ_fock, preferred_element_type=jnp.float32)
    singles_every = active[:, None] * (-singles_fock - 0.5 * coupling)
    sigma_singles = lax.dynamic_slice_in_dim(singles_every, root_index * local_roots, local_roots)
    singles_part = jnp.dot(
        singles_all.astype(jnp.float32), singles_every.T, precision=lax.Precision.HIGHEST
    )
    whole_matrix = doubles_part / math.sqrt(
        occ_count * occ_count * virt_count
    ) + singles_part / math.sqrt(occ_count)
    subspace = lax.dynamic_slice_in_dim(whole_matrix, root_index * local_roots, local_roots, 0)
    return (sigma_doubles, sigma_singles, subspace)


def solution(mesh):
    placed = (
        P("root", None),
        P("root", "virt", "occ"),
        P(),
        P(),
        P("occ", "virt", "root"),
        P("occ", "virt", "root"),
        P(),
    )
    return jax.shard_map(
        local,
        mesh=mesh,
        in_specs=placed,
        out_specs=(P("root", "virt", "occ"), P("root", None), P("root", None)),
        check_vma=False,
    )
```
